32 devices in a mesh: dp: 32 (over z, y, x, core), tensor: 1.
Axes of the slice: x: 2, y: 2, z: 4, core: 2. Of those that a mesh axis runs over, the one named last changes fastest.
Arguments:
- latent_raw: bfloat16 [6144, 512], P('dp'), may hold values from -6 to 6
- norm_gain: float32 [512], replicated, may hold values from 0.5 to 1.5
- up_weight: bfloat16 [512, 4096], P(None, 'tensor'), may hold values from -0.25 to 0.25
- grad_kv: bfloat16 [6144, 4096], P('dp', 'tensor'), may hold values from -3 to 3
Outputs:
- latent_grad: bfloat16 [6144, 512], P('dp')
- gain_grad: float32 [512], replicated
- weight_grad: float32 [512, 4096], P('dp', 'tensor')
The draws below stay inside these ranges and needn't reach their ends.
All inputs are finite; a program needn't handle non-finite values.
Results may differ from the reference program's by a relative error of at most 0.0029.
Values may be sent and summed in bfloat16 or wider, within the bound.
No kernel may reach another device: no remote copies, remote signals or barrier semaphores. Data moves between devices by JAX's collectives and lax.ppermute only.
A program may use at most 64 MiB of HBM per device.

```python
import jax
import jax.numpy as jnp
from jax import lax

KVL = 512
HEAD_DIM = 128
HEADS = 16
TOKENS = 6144


def strengthened(drawn, rng, source, target, blocks, factor):
    owner, partner = [(jnp.arange(drawn.shape[position]) // (drawn.shape[position] // blocks)).reshape([-1 if axis == position else 1 for axis in range(drawn.ndim)]) for position in (source, target)]
    chosen = jax.random.permutation(rng, blocks)[partner]
    strong = (owner == chosen) | (owner == (partner + blocks // 2) % blocks)
    return jnp.where(strong, factor * drawn, drawn)


def steps_of(rng, extent, shards, least, high):
    level = 1.0
    for position, parts in shards:
        draws = jax.random.uniform(jax.random.fold_in(jax.random.fold_in(rng, 6), position), (parts,), jnp.float32, least / len(shards), high / len(shards))
        level = level * jnp.repeat(jnp.exp(draws), extent[position] // parts).reshape((-1,) + (1,) * (len(extent) - 1 - position))
    return level


def noise(stream_key, shape, scale, bound, split=(), held_as=jnp.bfloat16):
    factor_of = steps_of(stream_key, shape, split, -0.22, 0.18) if split else 1.0
    entries = jax.random.normal(stream_key, shape, jnp.float32) * scale * factor_of
    return jnp.minimum(jnp.maximum(entries, -bound), bound).astype(held_as)


def bell_draw_with(stream_key, extent, spread, most, shards, heavy, dtype=jnp.bfloat16):
    array = spread * jax.random.normal(stream_key, extent, jnp.float32)
    if shards:
        array = array * steps_of(stream_key, extent, shards, -0.22, 0.18)
    return jnp.clip(strengthened(array, jax.random.fold_in(stream_key, 3), *heavy), -most, most).astype(dtype)


def setup_inputs(seed: int = 0) -> dict:
    arg_keys = jax.random.split(jax.random.key(seed), 5)
    return {
        "latent_raw": bell_draw_with(arg_keys[0], (TOKENS, KVL), 1.0, 6.0, ((0, 32),), (0, 1, 32, 2.75)),
        "norm_gain": jnp.clip(1.0 + 0.1 * jax.random.normal(arg_keys[1], (KVL,), jnp.float32), 0.5, 1.5),
        "up_weight": noise(arg_keys[2], (KVL, HEADS * 2 * HEAD_DIM), KVL ** -0.5, 0.25),
        "grad_kv": noise(arg_keys[3], (TOKENS, HEADS * 2 * HEAD_DIM), 0.5, 3.0, ((0, 32),)),
    }


epsilon = 1e-06

def reference(latent_raw, norm_gain, up_weight, grad_kv):
    latent_full = latent_raw.astype(jnp.float32)
    inverse = lax.rsqrt(lax.optimization_barrier(jnp.mean(latent_full * latent_full, axis=-1, keepdims=True)) + epsilon)
    scaled_rows = latent_full * inverse
    normed = (scaled_rows * norm_gain).astype(jnp.bfloat16)
    factor = float(TOKENS) ** (-0.5)
    grad_norm = lax.dot_general(grad_kv, up_weight, (((1,), (1,)), ((), ())), preferred_element_type=jnp.float32)
    gain_grad = lax.optimization_barrier(jnp.sum(grad_norm * scaled_rows, axis=0)) * factor
    upstream = grad_norm * norm_gain
    centred = upstream - scaled_rows * lax.optimization_barrier(jnp.mean(upstream * scaled_rows, axis=-1, keepdims=True))
    latent_grad = (inverse * centred).astype(jnp.bfloat16)
    weight_grad = lax.dot_general(normed, grad_kv, (((0,), (0,)), ((), ())), preferred_element_type=jnp.float32) * factor
    return (latent_grad, gain_grad, weight_grad)
```

```python
import jax
import jax.numpy as jnp
import numpy as np
from jax import lax
from jax.sharding import PartitionSpec as P

epsilon = 1e-06
lane = 128
narrow_steps = 4


def normalize(latent_raw):
    latent_full = latent_raw.astype(jnp.float32)
    inverse = lax.rsqrt(jnp.mean(latent_full * latent_full, axis=-1, keepdims=True) + epsilon)
    return (latent_full * inverse, inverse)


def norm_backward(grad_norm, scaled_rows, inverse, norm_gain):
    upstream = grad_norm * norm_gain
    centred = upstream - scaled_rows * jnp.mean(upstream * scaled_rows, axis=-1, keepdims=True)
    return (inverse * centred).astype(jnp.bfloat16)


def swap(value, mask):
    size = lax.axis_size("dp")
    return lax.ppermute(value, "dp", [(i, i ^ mask) for i in range(size)])


def chunk_orders(bit_count):
    low = list(range(1, min(bit_count, 4)))
    high = list(range(len(low) + 1, bit_count))
    turns = [low[k:] + low[:k] for k in range(len(low))]
    return [turn + high for turn in turns]


def column_cuts(columns, parts):
    blocks = columns // lane
    cuts = [(blocks * k + parts - 1) // parts * lane for k in range(parts)]
    return cuts + [columns]


def selector(me, order, rows, per):
    count = 1 << len(order)
    relative = np.zeros(count, np.int32)
    for place, bit in enumerate(order):
        relative |= ((np.arange(count) >> (len(order) - 1 - place)) & 1).astype(np.int32) << bit
    relative = jnp.asarray(np.repeat(relative, per))
    within = jnp.asarray(np.tile(np.arange(per, dtype=np.int32), count))
    wanted = (me ^ relative) * per + within
    return (lax.broadcasted_iota(jnp.int32, (rows, count * per), 0) == wanted[None, :]).astype(jnp.bfloat16)


def over_tokens(left, right):
    return lax.dot_general(left, right, (((0,), (0,)), ((), ())), preferred_element_type=jnp.float32)


def weight_gradient(normed, grad_kv, other_normed, other_grad):
    size = lax.axis_size("dp")
    bit_count = size.bit_length() - 1
    me = lax.axis_index("dp")
    rows = normed.shape[1]
    per = rows // size
    orders = chunk_orders(bit_count)
    cuts = column_cuts(grad_kv.shape[1], len(orders))
    pieces = []
    for chunk, order in enumerate(orders):
        pick = selector(me, order, rows, per)
        left = jnp.dot(normed, pick, preferred_element_type=jnp.float32).astype(jnp.bfloat16)
        other_left = jnp.dot(other_normed, pick, preferred_element_type=jnp.float32).astype(jnp.bfloat16)
        right = grad_kv[:, cuts[chunk]:cuts[chunk + 1]]
        other_right = other_grad[:, cuts[chunk]:cuts[chunk + 1]]
        half = left.shape[1] // 2
        away = over_tokens(left[:, half:], right) + over_tokens(other_left[:, half:], other_right)
        kept = over_tokens(left[:, :half], right) + over_tokens(other_left[:, :half], other_right)
        pieces.append((kept, away))
    for step in range(bit_count - 1):
        moved = []
        for order, (kept, away) in zip(orders, pieces):
            if step < narrow_steps:
                away = away.astype(jnp.bfloat16)
            moved.append(swap(away, 1 << order[step]))
        following = []
        for (kept, away), came in zip(pieces, moved):
            total = kept + came.astype(jnp.float32)
            half = total.shape[0] // 2
            following.append((total[:half], total[half:]) if step < bit_count - 2 else (total, None))
        pieces = following
    return jnp.concatenate([total for total, _ in pieces], axis=1)


def all_sum(value):
    size = lax.axis_size("dp")
    mask = 1
    while mask < size:
        value = value + swap(value, mask)
        mask *= 2
    return value


def per_device(latent_raw, norm_gain, up_weight, grad_kv):
    size = lax.axis_size("dp")
    paired = size >= 8 and size & (size - 1) == 0 and latent_raw.shape[1] % size == 0
    if paired:
        other_latent = swap(latent_raw, 1)
        other_grad = swap(grad_kv, 1)
    scaled_rows, inverse = normalize(latent_raw)
    normed = (scaled_rows * norm_gain).astype(jnp.bfloat16)
    factor = float(latent_raw.shape[0] * size) ** (-0.5)
    if paired:
        other_normed = (normalize(other_latent)[0] * norm_gain).astype(jnp.bfloat16)
        weight_sum = weight_gradient(normed, grad_kv, other_normed, other_grad)
    else:
        weight_sum = lax.psum_scatter(over_tokens(normed, grad_kv), "dp", scatter_dimension=0, tiled=True)
    partial_norm = lax.dot_general(
        grad_kv, up_weight, (((1,), (1,)), ((), ())), preferred_element_type=jnp.float32
    )
    grad_norm = lax.psum_scatter(partial_norm, "tensor", scatter_dimension=0, tiled=True)
    row_count = grad_norm.shape[0]
    offset = lax.axis_index("tensor") * row_count
    scaled_part = lax.dynamic_slice_in_dim(scaled_rows, offset, row_count, 0)
    inverse_part = lax.dynamic_slice_in_dim(inverse, offset, row_count, 0)
    gain_local = jnp.sum(grad_norm * scaled_part, axis=0)
    latent_part = norm_backward(grad_norm, scaled_part, inverse_part, norm_gain)
    latent_grad = lax.all_gather(latent_part, "tensor", axis=0, tiled=True)
    if lax.axis_size("tensor") > 1:
        gain_local = lax.psum(gain_local, "tensor")
    gain_grad = (all_sum(gain_local) if paired else lax.psum(gain_local, "dp")) * factor
    return (latent_grad, gain_grad, weight_sum * factor)


def solution(mesh):
    in_specs = (P("dp", None), P(), P(None, "tensor"), P("dp", "tensor"))
    out_specs = (P("dp", None), P(), P("dp", "tensor"))
    return jax.shard_map(
        per_device, mesh=mesh, in_specs=in_specs, out_specs=out_specs, check_vma=False
    )
```

```python
import jax
import jax.numpy as jnp
import numpy as np
from jax import lax
from jax.experimental import pallas as pl
from jax.experimental.pallas import tpu as pltpu
from jax.sharding import PartitionSpec as P

epsilon = 1e-06
lane = 128
narrow_steps = 4


def normalize(latent_raw):
    latent_full = latent_raw.astype(jnp.float32)
    inverse = lax.rsqrt(jnp.mean(latent_full * latent_full, axis=-1, keepdims=True) + epsilon)
    return (latent_full * inverse, inverse)


def norm_backward(grad_norm, scaled_rows, inverse, norm_gain):
    upstream = grad_norm * norm_gain
    centred = upstream - scaled_rows * jnp.mean(upstream * scaled_rows, axis=-1, keepdims=True)
    return (inverse * centred).astype(jnp.bfloat16)


def swap(value, mask):
    size = lax.axis_size("dp")
    return lax.ppermute(value, "dp", [(i, i ^ mask) for i in range(size)])


def chunk_orders(bit_count):
    low = list(range(1, min(bit_count, 4)))
    high = list(range(len(low) + 1, bit_count))
    turns = [low[k:] + low[:k] for k in range(len(low))]
    return [turn + high for turn in turns]


def column_cuts(columns, parts):
    blocks = columns // lane
    cuts = [-(-blocks * k // parts) * lane for k in range(parts)]
    return cuts + [columns]


def selector(me, order, rows, per):
    count = 1 << len(order)
    relative = np.zeros(count, np.int32)
    for place, bit in enumerate(order):
        relative |= ((np.arange(count) >> (len(order) - 1 - place)) & 1).astype(np.int32) << bit
    relative = jnp.asarray(np.repeat(relative, per))
    within = jnp.asarray(np.tile(np.arange(per, dtype=np.int32), count))
    wanted = (me ^ relative) * per + within
    return (lax.broadcasted_iota(jnp.int32, (rows, count * per), 0) == wanted[None, :]).astype(jnp.bfloat16)


def over_tokens(left, right):
    return lax.dot_general(left, right, (((0,), (0,)), ((), ())), preferred_element_type=jnp.float32)


def norm_kernel(latent_ref, gain_ref, weight_ref, grad_ref, latent_grad_ref, gain_sum_ref, normed_ref, total_ref):
    step = pl.program_id(0)
    product = lax.dot_general(
        grad_ref[...], weight_ref[...], (((1,), (1,)), ((), ())), preferred_element_type=jnp.float32
    )

    @pl.when(step == 0)
    def _():
        total_ref[...] = product

    @pl.when(step > 0)
    def _():
        total_ref[...] += product

    @pl.when(step == pl.num_programs(0) - 1)
    def _():
        scaled_rows, inverse = normalize(latent_ref[...])
        gain = gain_ref[...]
        grad_norm = total_ref[...]
        normed_ref[...] = (scaled_rows * gain).astype(jnp.bfloat16)
        gain_sum_ref[...] = jnp.sum(grad_norm * scaled_rows, axis=0, keepdims=True)
        latent_grad_ref[...] = norm_backward(grad_norm, scaled_rows, inverse, gain)


def norm_part(latent_raw, norm_gain, up_weight, grad_kv):
    tokens, width = latent_raw.shape
    columns = grad_kv.shape[1]
    steps = 4
    block = columns // steps
    latent_grad, gain_sum, normed = pl.pallas_call(
        norm_kernel,
        grid=(steps,),
        in_specs=[
            pl.BlockSpec((tokens, width), lambda k: (0, 0)),
            pl.BlockSpec((1, width), lambda k: (0, 0)),
            pl.BlockSpec((width, block), lambda k: (0, k)),
            pl.BlockSpec((tokens, block), lambda k: (0, k)),
        ],
        out_specs=[
            pl.BlockSpec((tokens, width), lambda k: (0, 0)),
            pl.BlockSpec((1, width), lambda k: (0, 0)),
            pl.BlockSpec((tokens, width), lambda k: (0, 0)),
        ],
        out_shape=[
            jax.ShapeDtypeStruct((tokens, width), jnp.bfloat16),
            jax.ShapeDtypeStruct((1, width), jnp.float32),
            jax.ShapeDtypeStruct((tokens, width), jnp.bfloat16),
        ],
        scratch_shapes=[pltpu.VMEM((tokens, width), jnp.float32)],
    )(latent_raw, norm_gain[None, :], up_weight, grad_kv)
    return latent_grad, gain_sum[0], normed


def split_float(value):
    parts = []
    for _ in range(3):
        part = lax.reduce_precision(value, 8, 7)
        parts.append(part)
        value = value - part
    return parts


def swap_with(away, value, mask):
    parts = split_float(value) if away.dtype == jnp.bfloat16 else [value]
    extra = jnp.concatenate(parts).reshape(-1, lane)
    used = extra.shape[0]
    if used > away.shape[0]:
        return swap(away, mask), value + swap(value, mask)
    extra = jnp.pad(extra, ((0, away.shape[0] - used), (0, 0))).astype(away.dtype)
    came = swap(jnp.concatenate([away, extra], axis=1), mask)
    columns = away.shape[1]
    theirs = came[:used, columns:].astype(jnp.float32).reshape(len(parts), -1)
    mine = parts[0]
    other = theirs[0]
    for k in range(1, len(parts)):
        mine = mine + parts[k]
        other = other + theirs[k]
    return came[:, :columns], mine + other


def weight_gradient(normed, grad_kv, other_normed, other_grad, gain_local):
    size = lax.axis_size("dp")
    bit_count = size.bit_length() - 1
    me = lax.axis_index("dp")
    rows = normed.shape[1]
    per = rows // size
    orders = chunk_orders(bit_count)
    cuts = column_cuts(grad_kv.shape[1], len(orders))
    pieces = []
    for chunk, order in enumerate(orders):
        pick = selector(me, order, rows, per)
        left = jnp.dot(normed, pick, preferred_element_type=jnp.float32).astype(jnp.bfloat16)
        other_left = jnp.dot(other_normed, pick, preferred_element_type=jnp.float32).astype(jnp.bfloat16)
        right = grad_kv[:, cuts[chunk]:cuts[chunk + 1]]
        other_right = other_grad[:, cuts[chunk]:cuts[chunk + 1]]
        half = left.shape[1] // 2
        away = over_tokens(left[:, half:], right) + over_tokens(other_left[:, half:], other_right)
        kept = over_tokens(left[:, :half], right) + over_tokens(other_left[:, :half], other_right)
        pieces.append((kept, away))
    for step in range(bit_count - 1):
        moved = []
        for chunk, (order, (kept, away)) in enumerate(zip(orders, pieces)):
            if step < narrow_steps:
                away = away.astype(jnp.bfloat16)
            mask = 1 << order[step]
            if chunk == len(orders) - 1:
                came, gain_local = swap_with(away, gain_local, mask)
            else:
                came = swap(away, mask)
            moved.append(came)
        following = []
        for (kept, away), came in zip(pieces, moved):
            total = kept + came.astype(jnp.float32)
            half = total.shape[0] // 2
            following.append((total[:half], total[half:]) if step < bit_count - 2 else (total, None))
        pieces = following
    return jnp.concatenate([total for total, _ in pieces], axis=1), gain_local


def per_device(latent_raw, norm_gain, up_weight, grad_kv):
    size = lax.axis_size("dp")
    paired = size >= 8 and size & (size - 1) == 0 and latent_raw.shape[1] % size == 0
    if paired:
        other_latent = swap(latent_raw, 1)
        other_grad = swap(grad_kv, 1)
    factor = float(latent_raw.shape[0] * size) ** (-0.5)
    if lax.axis_size("tensor") == 1 and grad_kv.shape[1] % (4 * lane) == 0:
        latent_grad, gain_local, normed = norm_part(latent_raw, norm_gain, up_weight, grad_kv)
    else:
        scaled_rows, inverse = normalize(latent_raw)
        normed = (scaled_rows * norm_gain).astype(jnp.bfloat16)
        partial_norm = lax.dot_general(
            grad_kv, up_weight, (((1,), (1,)), ((), ())), preferred_element_type=jnp.float32
        )
        grad_norm = lax.psum_scatter(partial_norm, "tensor", scatter_dimension=0, tiled=True)
        row_count = grad_norm.shape[0]
        offset = lax.axis_index("tensor") * row_count
        scaled_part = lax.dynamic_slice_in_dim(scaled_rows, offset, row_count, 0)
        inverse_part = lax.dynamic_slice_in_dim(inverse, offset, row_count, 0)
        gain_local = lax.psum(jnp.sum(grad_norm * scaled_part, axis=0), "tensor")
        latent_part = norm_backward(grad_norm, scaled_part, inverse_part, norm_gain)
        latent_grad = lax.all_gather(latent_part, "tensor", axis=0, tiled=True)
    if paired:
        other_normed = (normalize(other_latent)[0] * norm_gain).astype(jnp.bfloat16)
        gain_local = gain_local + swap(gain_local, 1)
        weight_sum, gain_sum = weight_gradient(normed, grad_kv, other_normed, other_grad, gain_local)
    else:
        weight_sum = lax.psum_scatter(over_tokens(normed, grad_kv), "dp", scatter_dimension=0, tiled=True)
        gain_sum = lax.psum(gain_local, "dp")
    return (latent_grad, gain_sum * factor, weight_sum * factor)


def solution(mesh):
    in_specs = (P("dp", None), P(), P(None, "tensor"), P("dp", "tensor"))
    out_specs = (P("dp", None), P(), P("dp", "tensor"))
    return jax.shard_map(
        per_device, mesh=mesh, in_specs=in_specs, out_specs=out_specs, check_vma=False
    )
```

```python
import jax
import jax.numpy as jnp
from jax import lax
from jax.experimental import pallas as pl
from jax.experimental.pallas import tpu as pltpu
from jax.sharding import PartitionSpec as P


epsilon = 1e-06
lane = 128
narrow_steps = 4


def normalize(latent_raw):
    latent_full = latent_raw.astype(jnp.float32)
    inverse = lax.rsqrt(jnp.mean(latent_full * latent_full, axis=-1, keepdims=True) + epsilon)
    return (latent_full * inverse, inverse)


def norm_backward(grad_norm, scaled_rows, inverse, norm_gain):
    upstream = grad_norm * norm_gain
    centred = upstream - scaled_rows * jnp.mean(upstream * scaled_rows, axis=-1, keepdims=True)
    return (inverse * centred).astype(jnp.bfloat16)


def swap(value, mask):
    size = lax.axis_size("dp")
    return lax.ppermute(value, "dp", [(i, i ^ mask) for i in range(size)])


def chunk_orders(bit_count):
    low = list(range(1, min(bit_count, 4)))
    high = list(range(len(low) + 1, bit_count))
    turns = [low[k:] + low[:k] for k in range(len(low))]
    return [turn + high for turn in turns]


def column_cuts(columns, parts):
    blocks = columns // lane
    cuts = [blocks * k // parts * lane for k in range(parts)]
    return cuts + [columns]


def selector(me, order, rows, per):
    shape = (rows, per << len(order))
    place = lax.broadcasted_iota(jnp.int32, shape, 1)
    block = place // per
    relative = jnp.zeros(shape, jnp.int32)
    for position, bit in enumerate(order):
        relative |= ((block >> (len(order) - 1 - position)) & 1) << bit
    wanted = (me ^ relative) * per + place % per
    return (lax.broadcasted_iota(jnp.int32, shape, 0) == wanted).astype(jnp.bfloat16)


def over_tokens(left, right):
    return lax.dot_general(left, right, (((0,), (0,)), ((), ())), preferred_element_type=jnp.float32)


def norm_kernel(latent_ref, gain_ref, weight_ref, grad_ref, latent_grad_ref, gain_sum_ref, total_ref):
    step = pl.program_id(0)
    product = lax.dot_general(
        grad_ref[...], weight_ref[...], (((1,), (1,)), ((), ())), preferred_element_type=jnp.float32
    )

    @pl.when(step == 0)
    def _():
        total_ref[...] = product

    @pl.when(step > 0)
    def _():
        total_ref[...] += product

    @pl.when(step == pl.num_programs(0) - 1)
    def _():
        scaled_rows, inverse = normalize(latent_ref[...])
        gain = gain_ref[...]
        grad_norm = total_ref[...]
        gain_sum_ref[...] = jnp.sum(grad_norm * scaled_rows, axis=0, keepdims=True)
        latent_grad_ref[...] = norm_backward(grad_norm, scaled_rows, inverse, gain)


def norm_part(latent_raw, norm_gain, up_weight, grad_kv):
    tokens, width = latent_raw.shape
    columns = grad_kv.shape[1]
    steps = 4
    block = columns // steps
    room = 4 * (width + tokens) * block + 32 * tokens * width + (1 << 21)
    latent_grad, gain_sum = pl.pallas_call(
        norm_kernel,
        grid=(steps,),
        in_specs=[
            pl.BlockSpec((tokens, width), lambda k: (0, 0)),
            pl.BlockSpec((1, width), lambda k: (0, 0)),
            pl.BlockSpec((width, block), lambda k: (0, k)),
            pl.BlockSpec((tokens, block), lambda k: (0, k)),
        ],
        out_specs=[
            pl.BlockSpec((tokens, width), lambda k: (0, 0)),
            pl.BlockSpec((1, width), lambda k: (0, 0)),
        ],
        out_shape=[
            jax.ShapeDtypeStruct((tokens, width), jnp.bfloat16),
            jax.ShapeDtypeStruct((1, width), jnp.float32),
        ],
        scratch_shapes=[pltpu.VMEM((tokens, width), jnp.float32)],
        compiler_params=pltpu.CompilerParams(vmem_limit_bytes=room),
    )(latent_raw, norm_gain[None, :], up_weight, grad_kv)
    return latent_grad, gain_sum[0]


def split_float(value):
    parts = []
    for _ in range(3):
        part = lax.reduce_precision(value, 8, 7)
        parts.append(part)
        value = value - part
    return parts


def swap_with(away, value, mask):
    parts = split_float(value) if away.dtype == jnp.bfloat16 else [value]
    extra = jnp.concatenate(parts).reshape(-1, lane)
    used = extra.shape[0]
    if used > away.shape[0]:
        return swap(away, mask), value + swap(value, mask)
    extra = jnp.pad(extra, ((0, away.shape[0] - used), (0, 0))).astype(away.dtype)
    came = swap(jnp.concatenate([away, extra], axis=1), mask)
    columns = away.shape[1]
    theirs = came[:used, columns:].astype(jnp.float32).reshape(len(parts), -1)
    mine = parts[0]
    other = theirs[0]
    for k in range(1, len(parts)):
        mine = mine + parts[k]
        other = other + theirs[k]
    return came[:, :columns], mine + other


def first_pieces(normed, grad_kv, other_normed, other_grad, orders):
    size = lax.axis_size("dp")
    me = lax.axis_index("dp")
    rows = normed.shape[1]
    cuts = column_cuts(grad_kv.shape[1], len(orders))
    pieces = []
    for chunk, order in enumerate(orders):
        pick = selector(me, order, rows, rows // size)
        left = jnp.dot(normed, pick, preferred_element_type=jnp.float32).astype(jnp.bfloat16)
        other_left = jnp.dot(other_normed, pick, preferred_element_type=jnp.float32).astype(jnp.bfloat16)
        right = grad_kv[:, cuts[chunk]:cuts[chunk + 1]]
        other_right = other_grad[:, cuts[chunk]:cuts[chunk + 1]]
        half = left.shape[1] // 2
        away = over_tokens(left[:, half:], right) + over_tokens(other_left[:, half:], other_right)
        kept = over_tokens(left[:, :half], right) + over_tokens(other_left[:, :half], other_right)
        pieces.append((kept, away.astype(jnp.bfloat16)))
    return pieces


def halve(pieces, moved):
    following = []
    for (kept, _), came in zip(pieces, moved):
        total = kept + came.astype(jnp.float32)
        half = total.shape[0] // 2
        following.append((total[:half], total[half:]))
    return following


def later_steps(pieces, orders, gain_local):
    steps = len(orders[0])
    for step in range(1, steps):
        moved = []
        for chunk, (order, (kept, away)) in enumerate(zip(orders, pieces)):
            if step < narrow_steps:
                away = away.astype(jnp.bfloat16)
            mask = 1 << order[step]
            if chunk == 0:
                came, gain_local = swap_with(away, gain_local, mask)
            else:
                came = swap(away, mask)
            moved.append(came)
        if step < steps - 1:
            pieces = halve(pieces, moved)
    totals = [kept + came.astype(jnp.float32) for (kept, _), came in zip(pieces, moved)]
    return jnp.concatenate(totals, axis=1), gain_local


def per_device(latent_raw, norm_gain, up_weight, grad_kv):
    size = lax.axis_size("dp")
    paired = size >= 8 and size & (size - 1) == 0 and latent_raw.shape[1] % size == 0
    if paired:
        other_latent = swap(latent_raw, 1)
        other_grad = swap(grad_kv, 1)
    factor = float(latent_raw.shape[0] * size) ** (-0.5)
    scaled_rows, inverse = normalize(latent_raw)
    normed = (scaled_rows * norm_gain).astype(jnp.bfloat16)
    late_gain = norm_gain
    if paired:
        orders = chunk_orders(size.bit_length() - 1)
        other_normed = (normalize(other_latent)[0] * norm_gain).astype(jnp.bfloat16)
        pieces = first_pieces(normed, grad_kv, other_normed, other_grad, orders)
        moved = []
        for order, (_, away) in zip(orders, pieces):
            moved.append(swap(away, 1 << order[0]))
        late_gain, _ = lax.optimization_barrier((norm_gain, tuple(away for _, away in pieces)))
    if lax.axis_size("tensor") == 1 and grad_kv.shape[1] % (4 * lane) == 0:
        latent_grad, gain_local = norm_part(latent_raw, late_gain, up_weight, grad_kv)
    else:
        partial_norm = lax.dot_general(
            grad_kv, up_weight, (((1,), (1,)), ((), ())), preferred_element_type=jnp.float32
        )
        grad_norm = lax.psum_scatter(partial_norm, "tensor", scatter_dimension=0, tiled=True)
        row_count = grad_norm.shape[0]
        offset = lax.axis_index("tensor") * row_count
        scaled_part = lax.dynamic_slice_in_dim(scaled_rows, offset, row_count, 0)
        inverse_part = lax.dynamic_slice_in_dim(inverse, offset, row_count, 0)
        gain_local = lax.psum(jnp.sum(grad_norm * scaled_part, axis=0), "tensor")
        latent_part = norm_backward(grad_norm, scaled_part, inverse_part, late_gain)
        latent_grad = lax.all_gather(latent_part, "tensor", axis=0, tiled=True)
    if paired:
        gain_local = gain_local + swap(gain_local, 1)
        gain_local = gain_local + swap(gain_local, 1 << orders[0][0])
        weight_sum, gain_sum = later_steps(halve(pieces, moved), orders, gain_local)
    else:
        weight_sum = lax.psum_scatter(over_tokens(normed, grad_kv), "dp", scatter_dimension=0, tiled=True)
        gain_sum = lax.psum(gain_local, "dp")
    return (latent_grad, gain_sum * factor, weight_sum * factor)


def solution(mesh):
    in_specs = (P("dp", None), P(), P(None, "tensor"), P("dp", "tensor"))
    out_specs = (P("dp", None), P(), P("dp", "tensor"))

    return jax.shard_map(per_device, mesh=mesh, in_specs=in_specs, out_specs=out_specs, check_vma=False)
```
